32 devices in a mesh: res: 8 (over z, y), seq: 4 (over x, core).
Axes of the slice: x: 2, y: 2, z: 4, core: 2. Of those that a mesh axis runs over, the one named last changes fastest.
Arguments:
- alignment: bfloat16 [384, 256, 256], P('seq', 'res'), may hold values from -6 to 6
- query_weight: bfloat16 [256, 256], replicated, may hold values from -1 to 1
- w_keyval: bfloat16 [256, 512], replicated, may hold values from -0.375 to 0.375
- w_gate: bfloat16 [256, 256], replicated, may hold values from -0.375 to 0.375
- output_weight: bfloat16 [256, 256], replicated, may hold values from -0.75 to 0.75
- w_factors: bfloat16 [256, 64], replicated, may hold values from -1.5 to 1.5
- w_pair_out: bfloat16 [1024, 128], replicated, may hold values from -0.1875 to 0.1875
Outputs:
- alignment_update: bfloat16 [384, 256, 256], P('seq', 'res')
- pair_representation_update: bfloat16 [256, 256, 128], P(('res', 'seq'))
The draws below stay inside these ranges and needn't reach their ends.
All inputs are finite; a program needn't handle non-finite values.
Results may differ from the reference program's by a relative error of at most 0.012.
The reference program's roundings to bfloat16 on the way count: a program that leaves them out, or rounds other values in their place, can miss the bound.
Values may be sent and summed in bfloat16 or wider, within the bound.
A program may use at most 256 MiB of HBM per device.

```python
import math
import jax
import jax.numpy as jnp
from jax import lax

D = 256
P_SIZE = 128
HEADS = 8
HC = 32
C = 32
HD = 256
S = 384
R = 256


def levels(own_key, dims, pieces, low, largest):
    gain, own = 1.0, jax.random.fold_in(own_key, 6)
    for position, shards_of in pieces:
        draws = jnp.exp(jax.random.uniform(jax.random.fold_in(own, position), (shards_of,), jnp.float32, low / len(pieces), largest / len(pieces)))
        gain = gain * jnp.repeat(draws, dims[position] // shards_of).reshape([-1 if axis == position else 1 for axis in range(len(dims))])
    return gain


def bell_draw(rng, shape, deviation, bound, pieces=(), held_as=jnp.bfloat16):
    drawn = deviation * jax.random.normal(rng, shape, jnp.float32)
    if pieces:
        drawn = drawn * levels(rng, shape, pieces, -0.22, 0.18)
    return jnp.clip(drawn, -bound, bound).astype(held_as)


def setup_inputs(seed: int = 0) -> dict:
    key_list = jax.random.split(jax.random.key(seed), 8)
    return {
        "alignment": bell_draw(key_list[0], (S, R, D), 1.0, 6.0, ((0, 4), (1, 8))),
        "query_weight": bell_draw(key_list[1], (D, HD), (D // 9) ** -0.5, 1.0),
        "w_keyval": bell_draw(key_list[2], (D, 2 * HD), D ** -0.5, 0.375),
        "w_gate": bell_draw(key_list[3], (D, HD), D ** -0.5, 0.375),
        "output_weight": bell_draw(key_list[4], (HD, D), (HD // 4) ** -0.5, 0.75),
        "w_factors": bell_draw(key_list[5], (D, 2 * C), (D // 16) ** -0.5, 1.5),
        "w_pair_out": bell_draw(key_list[6], (C * C, P_SIZE), (C * C) ** -0.5, 0.1875),
    }


def normalize(alignment):
    values = alignment.astype(jnp.float32)
    centered = values - lax.optimization_barrier(jnp.mean(values, axis=-1, keepdims=True))
    spread = lax.optimization_barrier(jnp.mean(centered * centered, axis=-1, keepdims=True))
    return (centered * lax.rsqrt(spread + 1e-05)).astype(jnp.bfloat16)

def reference(alignment, query_weight, w_keyval, w_gate, output_weight, w_factors, w_pair_out):
    normed = normalize(alignment)
    queries = jnp.dot(normed, query_weight, preferred_element_type=jnp.float32).astype(jnp.bfloat16)
    keyvals = jnp.dot(normed, w_keyval, preferred_element_type=jnp.float32).astype(jnp.bfloat16)
    gating = jax.nn.sigmoid(jnp.dot(normed, w_gate, preferred_element_type=jnp.float32))
    hidden = HEADS * HC
    seq_total = normed.shape[0]
    residues = normed.shape[1]
    group_size = math.gcd(residues, 8)

    def attend_block(block_index):
        start_row = (block_index * group_size).astype(jnp.int32)
        query_block = lax.dynamic_slice_in_dim(queries, start_row, group_size, 1).astype(jnp.float32)
        keyval_block = lax.dynamic_slice_in_dim(keyvals, start_row, group_size, 1).astype(jnp.float32)
        per_head_query = query_block.reshape(seq_total, group_size, HEADS, HC)
        head_keys = keyval_block[:, :, :hidden].reshape(seq_total, group_size, HEADS, HC)
        head_values = keyval_block[:, :, hidden:].reshape(seq_total, group_size, HEADS, HC)
        scores = jnp.einsum('qrhd,krhd->rhqk', per_head_query, head_keys) / math.sqrt(HC)
        exponent = jnp.exp(scores)
        weights = exponent.astype(jnp.bfloat16).astype(jnp.float32)
        denominators = jnp.transpose(lax.optimization_barrier(jnp.sum(exponent, axis=-1)), (2, 0, 1))
        weighted = jnp.einsum('rhqk,krhd->qrhd', weights, head_values)
        return (weighted / denominators[:, :, :, None]).reshape(seq_total, group_size, hidden)
    blocks = lax.map(attend_block, jnp.arange(residues // group_size, dtype=jnp.int32))
    attended = jnp.transpose(blocks, (1, 0, 2, 3)).reshape(seq_total, residues, hidden)
    gated_output_rows = (gating * attended).astype(jnp.bfloat16)
    alignment_update = jnp.dot(gated_output_rows, output_weight, preferred_element_type=jnp.float32).astype(jnp.bfloat16)
    factors = jnp.dot(normed, w_factors, preferred_element_type=jnp.float32).astype(jnp.bfloat16)
    factor = factors.shape[2] // 2
    left_factor = factors[:, :, :factor].astype(jnp.float32).reshape(seq_total, residues * factor)
    right_factor = factors[:, :, factor:].astype(jnp.float32).reshape(seq_total, residues * factor)
    channels = w_pair_out.shape[1]
    pair_weight = w_pair_out.astype(jnp.float32).reshape(factor, factor, channels)
    row_block = math.gcd(residues, 32)

    def pair_block(block_index):
        start_col = (block_index * row_block * factor).astype(jnp.int32)
        left_rows = lax.dynamic_slice_in_dim(left_factor, start_col, row_block * factor, 1)
        products = lax.dot_general(left_rows, right_factor, (((0,), (0,)), ((), ())), precision=lax.Precision.HIGHEST, preferred_element_type=jnp.float32)
        products = (products * (1.0 / seq_total)).reshape(row_block, factor, residues, factor)
        return jnp.einsum('icje,cep->ijp', products, pair_weight, precision=lax.Precision.HIGHEST)
    pair_blocks = lax.map(pair_block, jnp.arange(residues // row_block, dtype=jnp.int32))
    pair_representation_update = pair_blocks.reshape(residues, residues, channels).astype(jnp.bfloat16)
    return (alignment_update, pair_representation_update)
```

```python
import math

import jax
import jax.numpy as jnp
from jax import lax
from jax.experimental import pallas as pl
from jax.experimental.pallas import tpu as pltpu
from jax.sharding import PartitionSpec as P

HEADS = 8
HC = 32
LOG2E = 1.4426950408889634
epsilon = 1e-05
NT = (((1,), (1,)), ((), ()))


def mm(a, b):
    return jnp.dot(a, b, preferred_element_type=jnp.float32)


def mm_nt(a, b):
    return lax.dot_general(a, b, NT, preferred_element_type=jnp.float32)


def normalize_kernel(x_ref, o_ref, scratch):
    seqs, residues, width = x_ref.shape
    step = 8

    def norm(i, carry):
        values = x_ref[pl.ds(i * step, step)].reshape(step * residues, width).astype(jnp.float32)
        centered = values - jnp.mean(values, axis=-1, keepdims=True)
        spread = jnp.mean(centered * centered, axis=-1, keepdims=True)
        normed = centered * lax.rsqrt(spread + epsilon)
        for part in range(width // 128):
            scratch[part, pl.ds(i * (step * residues), step * residues), :] = normed[
                :, part * 128 : (part + 1) * 128
            ]
        return carry

    lax.fori_loop(0, seqs // step, norm, 0)

    def move(r, carry):
        for part in range(width // 128):
            o_ref[r, :, part * 128 : (part + 1) * 128] = scratch[
                part, pl.ds(r, seqs, residues), :
            ].astype(jnp.bfloat16)
        return carry

    lax.fori_loop(0, residues, move, 0)


def attend_residues(own, everything, wqg, wkv, wout):
    groups, count, seqs, width = everything.shape
    hidden = HEADS * HC
    kv = mm(everything.reshape(groups * count * seqs, width), wkv).astype(jnp.bfloat16)
    kv = kv.reshape(groups, count, seqs, 2 * hidden)
    qg = mm(own.reshape(count * seqs, width), wqg)
    queries = qg[:, :hidden].astype(jnp.bfloat16)
    gating = jax.nn.sigmoid(qg[:, hidden:])
    head_of = lax.broadcasted_iota(jnp.int32, (seqs, hidden), 1) // HC
    gated = []
    for n in range(count):
        q = queries[n * seqs : (n + 1) * seqs].astype(jnp.float32)
        stacked = jnp.concatenate(
            [jnp.where(head_of == h, q, 0.0).astype(jnp.bfloat16) for h in range(HEADS)], axis=0
        )
        keys = kv[:, n, :, :hidden].reshape(groups * seqs, hidden)
        values = kv[:, n, :, hidden:].reshape(groups * seqs, hidden)
        exponent = jnp.exp2(mm_nt(stacked, keys) * (LOG2E / math.sqrt(HC)))
        inverse = 1.0 / jnp.sum(exponent, axis=-1, keepdims=True)
        weighted = mm(exponent.astype(jnp.bfloat16), values)
        attended = jnp.zeros((seqs, hidden), jnp.float32)
        for h in range(HEADS):
            rows = slice(h * seqs, (h + 1) * seqs)
            attended = jnp.where(head_of == h, weighted[rows] * inverse[rows], attended)
        gated.append((gating[n * seqs : (n + 1) * seqs] * attended).astype(jnp.bfloat16))
    return mm(jnp.concatenate(gated, axis=0), wout)


def attention_kernel(own_ref, all_ref, wqg_ref, wkv_ref, wout_ref, o_ref, scratch):
    step = pl.program_id(0)
    count, seqs, width = own_ref.shape
    residues = o_ref.shape[1]
    update = attend_residues(
        own_ref[...], all_ref[...], wqg_ref[...], wkv_ref[...], wout_ref[...]
    )
    for n in range(count):
        for part in range(width // 128):
            scratch[part, pl.ds(step * count + n, seqs, residues), :] = update[
                n * seqs : (n + 1) * seqs, part * 128 : (part + 1) * 128
            ]

    @pl.when(step == pl.num_programs(0) - 1)
    def _():
        chunk = 8

        def finish(i, carry):
            for part in range(width // 128):
                o_ref[pl.ds(i * chunk, chunk), :, part * 128 : (part + 1) * 128] = (
                    scratch[part, pl.ds(i * (chunk * residues), chunk * residues), :]
                    .astype(jnp.bfloat16)
                    .reshape(chunk, residues, 128)
                )
            return carry

        lax.fori_loop(0, seqs // chunk, finish, 0)


def factor_kernel(all_ref, wft_ref, left_ref, right_ref, scratch):
    step = pl.program_id(0)
    groups, count, seqs, width = all_ref.shape
    factor = wft_ref.shape[0] // 2
    residues = right_ref.shape[1]
    for n in range(count):
        both = mm_nt(wft_ref[...], all_ref[:, n].reshape(groups * seqs, width))
        left_ref[n] = both[:factor].astype(jnp.bfloat16)
        for part in range(groups * seqs // 128):
            scratch[part, pl.ds(step * count + n, factor, residues), :] = both[
                factor:, part * 128 : (part + 1) * 128
            ]

    @pl.when(step == pl.num_programs(0) - 1)
    def _():
        for part in range(groups * seqs // 128):
            right_ref[:, :, part * 128 : (part + 1) * 128] = (
                scratch[part].astype(jnp.bfloat16).reshape(factor, residues, 128)
            )


def pair_kernel(scaling, left_ref, right_ref, w_ref, o_ref, scratch):
    blocks, factor, residues, depth = right_ref.shape
    rows = o_ref.shape[0]
    channels = o_ref.shape[2]
    lanes = left_ref.shape[0]
    pack = 128 // factor
    span = blocks * residues
    for b in range(blocks):
        products = (
            mm_nt(right_ref[b].reshape(factor * residues, depth), left_ref[...]) * scaling
        ).astype(jnp.bfloat16)
        for e in range(factor):
            for g in range(lanes // 128):
                scratch[pl.ds(g * span + b * residues, residues), e * 128 : (e + 1) * 128] = (
                    products[e * residues : (e + 1) * residues, g * 128 : (g + 1) * 128]
                )
    pair = mm(scratch[...], w_ref[...])
    for i in range(rows):
        g, k = i // pack, i % pack
        o_ref[i] = pair[g * span : (g + 1) * span, k * channels : (k + 1) * channels].astype(
            jnp.bfloat16
        )


def whole(*shape):
    return pl.BlockSpec(shape, lambda i: (0,) * len(shape))


LIMIT = pltpu.CompilerParams(vmem_limit_bytes=60 * 1024 * 1024)


def per_device(alignment, query_weight, w_keyval, w_gate, output_weight, w_factors, w_pair_out):
    seqs, residues, width = alignment.shape
    groups = lax.axis_size("seq")
    blocks = lax.axis_size("res")
    depth = seqs * groups
    factor = w_factors.shape[1] // 2
    channels = w_pair_out.shape[1]
    hidden = query_weight.shape[1]
    own_rows = residues // groups

    normed = pl.pallas_call(
        normalize_kernel,
        out_shape=jax.ShapeDtypeStruct((residues, seqs, width), jnp.bfloat16),
        scratch_shapes=[pltpu.VMEM((width // 128, seqs * residues, 128), jnp.float32)],
        compiler_params=LIMIT,
        name="normalize",
    )(alignment)
    everything = lax.all_gather(normed, "seq", axis=0, tiled=False)

    count = 4
    wft = jnp.transpose(w_factors)
    left, right = pl.pallas_call(
        factor_kernel,
        grid=(residues // count,),
        in_specs=[
            pl.BlockSpec((groups, count, seqs, width), lambda i: (0, i, 0, 0)),
            whole(2 * factor, width),
        ],
        out_specs=[
            pl.BlockSpec((count, factor, depth), lambda i: (i, 0, 0)),
            whole(factor, residues, depth),
        ],
        out_shape=[
            jax.ShapeDtypeStruct((residues, factor, depth), jnp.bfloat16),
            jax.ShapeDtypeStruct((factor, residues, depth), jnp.bfloat16),
        ],
        scratch_shapes=[pltpu.VMEM((depth // 128, factor * residues, 128), jnp.float32)],
        compiler_params=LIMIT,
        name="factors",
    )(everything, wft)
    right_all = lax.all_gather(right, "res", axis=0, tiled=False)

    wqg = jnp.concatenate([query_weight, w_gate], axis=1)
    alignment_update = pl.pallas_call(
        attention_kernel,
        grid=(residues // count,),
        in_specs=[
            pl.BlockSpec((count, seqs, width), lambda i: (i, 0, 0)),
            pl.BlockSpec((groups, count, seqs, width), lambda i: (0, i, 0, 0)),
            whole(width, 2 * hidden),
            whole(width, 2 * hidden),
            whole(hidden, width),
        ],
        out_specs=whole(seqs, residues, width),
        out_shape=jax.ShapeDtypeStruct((seqs, residues, width), jnp.bfloat16),
        scratch_shapes=[pltpu.VMEM((width // 128, seqs * residues, 128), jnp.float32)],
        compiler_params=LIMIT,
        cost_estimate=pl.CostEstimate(
            flops=30_000_000_000, bytes_accessed=10_000_000, transcendentals=10_000_000
        ),
        name="attention",
    )(normed, everything, wqg, w_keyval, output_weight)

    pack = 128 // factor
    w = jnp.transpose(w_pair_out.reshape(factor, factor, channels), (1, 0, 2))
    eye = jnp.eye(pack, dtype=w.dtype)
    spread = (w[:, None, :, None, :] * eye[None, :, None, :, None]).reshape(
        factor * pack * factor, pack * channels
    )
    own_left = lax.dynamic_slice_in_dim(
        left, lax.axis_index("seq") * own_rows, own_rows, 0
    ).reshape(own_rows * factor, depth)
    each = math.gcd(blocks, 4)
    pair = pl.pallas_call(
        lambda *refs: pair_kernel(1.0 / depth, *refs),
        grid=(blocks // each,),
        in_specs=[
            whole(own_rows * factor, depth),
            pl.BlockSpec((each, factor, residues, depth), lambda i: (i, 0, 0, 0)),
            whole(*spread.shape),
        ],
        out_specs=pl.BlockSpec((own_rows, each * residues, channels), lambda i: (0, i, 0)),
        out_shape=jax.ShapeDtypeStruct((own_rows, blocks * residues, channels), jnp.bfloat16),
        scratch_shapes=[
            pltpu.VMEM((own_rows // pack * each * residues, factor * 128), jnp.bfloat16)
        ],
        compiler_params=LIMIT,
        name="pair",
    )(own_left, right_all, spread)
    return (alignment_update, pair)


def solution(mesh):
    in_specs = (P("seq", "res", None), P(), P(), P(), P(), P(), P())
    out_specs = (P("seq", "res", None), P(("res", "seq"), None, None))
    return jax.shard_map(
        per_device, mesh=mesh, in_specs=in_specs, out_specs=out_specs, check_vma=False
    )
```

```python
import functools
import math

import jax
import jax.numpy as jnp
from jax import lax
from jax.experimental import pallas as pl
from jax.experimental.pallas import tpu as pltpu
from jax.sharding import PartitionSpec as P

HEADS = 8
HC = 32
LOG2E = 1.4426950408889634
epsilon = 1e-05
NT = (((1,), (1,)), ((), ()))


def mm(a, b):
    return jnp.dot(a, b, preferred_element_type=jnp.float32)


def mm_nt(a, b):
    return lax.dot_general(a, b, NT, preferred_element_type=jnp.float32)


MESH = pl.DeviceIdType.MESH
COUNT = 4


def attend_residues(own, everything, wqg, wkv, wout):
    groups, count, seqs, width = everything.shape
    hidden = HEADS * HC
    kv = mm(everything.reshape(groups * count * seqs, width), wkv).astype(jnp.bfloat16)
    kv = kv.reshape(groups, count, seqs, 2 * hidden)
    qg = mm(own.reshape(count * seqs, width), wqg)
    queries = qg[:, :hidden].astype(jnp.bfloat16)
    gating = jax.nn.sigmoid(qg[:, hidden:])
    head_of = lax.broadcasted_iota(jnp.int32, (seqs, hidden), 1) // HC
    gated = []
    for n in range(count):
        q = queries[n * seqs : (n + 1) * seqs].astype(jnp.float32)
        stacked = jnp.concatenate(
            [jnp.where(head_of == h, q, 0.0).astype(jnp.bfloat16) for h in range(HEADS)], axis=0
        )
        keys = kv[:, n, :, :hidden].reshape(groups * seqs, hidden)
        values = kv[:, n, :, hidden:].reshape(groups * seqs, hidden)
        exponent = jnp.exp2(mm_nt(stacked, keys) * (LOG2E / math.sqrt(HC)))
        inverse = 1.0 / jnp.sum(exponent, axis=-1, keepdims=True)
        weighted = mm(exponent.astype(jnp.bfloat16), values)
        attended = jnp.zeros((seqs, hidden), jnp.float32)
        for h in range(HEADS):
            rows = slice(h * seqs, (h + 1) * seqs)
            attended = jnp.where(head_of == h, weighted[rows] * inverse[rows], attended)
        gated.append((gating[n * seqs : (n + 1) * seqs] * attended).astype(jnp.bfloat16))
    return mm(jnp.concatenate(gated, axis=0), wout)


def block_kernel(
    scaling,
    blocks,
    groups,
    x_ref,
    wqg_ref,
    wkv_ref,
    wout_ref,
    wft_ref,
    wpair_ref,
    o_ref,
    pair_ref,
    gathered,
    strided,
    factor_rows,
    left_all,
    right_all,
    outer,
    outgoing,
    incoming,
    cross_send,
    cross_recv,
    twin_send,
    twin_recv,
    relay_send,
    relay_recv,
    ring_send,
    ring_recv,
    share_send,
    share_recv,
    swap_send,
    swap_recv,
):
    seqs, residues, width = x_ref.shape
    depth = seqs * groups
    factor = wft_ref.shape[0] // 2
    own_rows = residues // groups
    channels = pair_ref.shape[2]
    half = residues // 2
    parts = residues // COUNT
    half_parts = parts // 2
    hops = blocks // 2
    r = lax.axis_index("res")
    q = lax.axis_index("seq")
    core = lax.rem(q, 2)
    side = q // 2
    twin = q + 1 - 2 * core
    across = lax.rem(q + 2, groups)
    twin_across = lax.rem(twin + 2, groups)

    def ring_of(block):
        z, y = block // 2, lax.rem(block, 2)
        return jnp.where(y == 0, z, blocks - 1 - z)

    def block_of(place):
        return jnp.where(place < blocks // 2, 2 * place, 2 * (blocks - 1 - place) + 1)

    place = ring_of(r)
    ahead = block_of(lax.rem(place + 1, blocks))
    behind = block_of(lax.rem(place + blocks - 1, blocks))

    barrier = pltpu.get_barrier_semaphore()
    for target in ((r, twin), (r, across), (ahead, q), (behind, q)):
        pl.semaphore_signal(barrier, inc=1, device_id=target, device_id_type=MESH)
    pl.semaphore_wait(barrier, 4)

    def part_at(p):
        return lax.rem(p + side * half_parts, parts)

    def rows_of(owner, part):
        return gathered.at[owner, pl.ds(part * COUNT, COUNT)]

    def send(ref, dst, send_sem, recv_sem, target):
        return pltpu.make_async_remote_copy(
            src_ref=ref,
            dst_ref=dst,
            send_sem=send_sem,
            recv_sem=recv_sem,
            device_id=target,
            device_id_type=MESH,
        )

    def cross(owner, p, part):
        block = rows_of(owner, part)
        return send(block, block, cross_send.at[p], cross_recv.at[p], (r, across))

    def direct(owner, p, part):
        block = rows_of(owner, part)
        return send(block, block, twin_send.at[p], twin_recv.at[p], (r, twin))

    def relay(owner, p, part):
        block = rows_of(owner, part)
        return send(block, block, relay_send.at[p], relay_recv.at[p], (r, twin))

    step = 8
    for turn in range(2):
        which = (1 - side) if turn == 0 else side
        base = pl.multiple_of(which * half, half)

        def norm(i, carry):
            values = (
                x_ref[pl.ds(i * step, step), pl.ds(base, half), :]
                .reshape(step * half, width)
                .astype(jnp.float32)
            )
            centered = values - jnp.mean(values, axis=-1, keepdims=True)
            spread = jnp.mean(centered * centered, axis=-1, keepdims=True)
            normed = centered * lax.rsqrt(spread + epsilon)
            for part in range(width // 128):
                strided[part, pl.ds(i * (step * half), step * half), :] = normed[
                    :, part * 128 : (part + 1) * 128
                ]
            return carry

        lax.fori_loop(0, seqs // step, norm, 0)

        def move(k, carry):
            for n in range(COUNT):
                for part in range(width // 128):
                    gathered[q, base + k * COUNT + n, :, part * 128 : (part + 1) * 128] = strided[
                        part, pl.ds(k * COUNT + n, seqs, half), :
                    ].astype(jnp.bfloat16)
            return carry

        def start_across(k, carry):
            cross(q, turn * half_parts + k, which * half_parts + k).start()
            return carry

        def move_and_start(k, carry):
            move(k, carry)
            return start_across(k, carry)

        lax.fori_loop(0, half_parts, move_and_start, 0)

    def start_twin(p, carry):
        direct(q, p, part_at(p)).start()
        return carry

    lax.fori_loop(0, parts, start_twin, 0)

    own_e = pl.ds(pl.multiple_of(core * (factor // 2), factor // 2), factor // 2)
    twin_e = pl.ds(pl.multiple_of((1 - core) * (factor // 2), factor // 2), factor // 2)

    def ring_copy(way, hop):
        shift = blocks - hop if way == 0 else hop
        block = block_of(lax.rem(place + shift, blocks))
        ref = right_all.at[block, own_e]
        return send(
            ref,
            ref,
            ring_send.at[way, hop],
            ring_recv.at[way, hop],
            ((ahead if way == 0 else behind), q),
        )

    def landed(way, hop):
        shift = blocks - hop - 1 if way == 0 else hop + 1
        return block_of(lax.rem(place + shift, blocks))

    def share_copy(way, hop, mine=True):
        ref = right_all.at[landed(way, hop), own_e if mine else twin_e]
        return send(ref, ref, share_send.at[way, hop], share_recv.at[way, hop], (r, twin))

    def arrive(way, hop):
        block = landed(way, hop)
        ref = right_all.at[block, own_e]
        send(
            ref, ref, ring_send.at[way, hop], ring_recv.at[way, hop], ((ahead if way == 0 else behind), q)
        ).wait_recv()

    ways = (hops, blocks - 1 - hops)

    def advance(hop):
        for way in range(2):

            @pl.when(hop <= ways[way])
            def _():
                @pl.when(hop > 0)
                def _():
                    arrive(way, hop - 1)

                @pl.when(hop < ways[way])
                def _():
                    ring_copy(way, hop).start()

                @pl.when(hop > 0)
                def _():
                    share_copy(way, hop - 1).start()

    def one_part(p, carry):
        part = part_at(p)
        cross(across, p, part).wait_recv()
        relay(across, p, part).start()
        direct(twin, p, part).wait_recv()
        relay(twin_across, p, part).wait_recv()
        everything = gathered[:, pl.ds(part * COUNT, COUNT)]
        for n in range(COUNT):
            both = mm_nt(wft_ref[...], everything[:, n].reshape(depth, width))
            left_all[part * COUNT + n] = both[:factor].astype(jnp.bfloat16)
            for piece in range(depth // 128):
                factor_rows[piece, pl.ds(p * COUNT + n, factor, residues), :] = both[
                    factor:, piece * 128 : (piece + 1) * 128
                ]

        @pl.when(p == half_parts - 1)
        def _():
            for e in range(factor):
                for piece in range(depth // 128):
                    right_all[r, e, :, piece * 128 : (piece + 1) * 128] = factor_rows[
                        piece, e * residues : e * residues + half, :
                    ].astype(jnp.bfloat16)

        update = attend_residues(
            gathered[q, pl.ds(part * COUNT, COUNT)],
            everything,
            wqg_ref[...],
            wkv_ref[...],
            wout_ref[...],
        )
        for n in range(COUNT):
            for piece in range(width // 128):
                strided[piece, pl.ds(part * COUNT + n, seqs, residues), :] = update[
                    n * seqs : (n + 1) * seqs, piece * 128 : (piece + 1) * 128
                ]

        @pl.when(p >= half_parts - 1)
        def _():
            advance(p - (half_parts - 1))

        return carry

    lax.fori_loop(0, parts, one_part, 0)

    def late(hop, carry):
        advance(hop)
        return carry

    lax.fori_loop(half_parts + 1, hops + 1, late, 0)

    def finish(i, carry):
        for piece in range(width // 128):
            o_ref[pl.ds(i * step, step), :, piece * 128 : (piece + 1) * 128] = (
                strided[piece, pl.ds(i * (step * residues), step * residues), :]
                .astype(jnp.bfloat16)
                .reshape(step, residues, 128)
            )
        return carry

    lax.fori_loop(0, seqs // step, finish, 0)

    for way in range(2):

        def shared(hop, carry):
            share_copy(way, hop, False).wait_recv()
            return carry

        lax.fori_loop(0, ways[way], shared, 0)

    pack = 128 // factor
    lanes = 2 * own_rows * factor
    left = jnp.concatenate(
        [
            left_all[pl.ds(q * own_rows, own_rows)].reshape(own_rows * factor, depth),
            left_all[pl.ds(across * own_rows, own_rows)].reshape(own_rows * factor, depth),
        ],
        axis=0,
    )
    each = outer.shape[0] // (lanes // 128) // half
    span = each * half
    turns = blocks // each

    def swap_copy(t):
        return send(
            outgoing.at[t], incoming.at[t], swap_send.at[t], swap_recv.at[t], (r, across)
        )

    def one_turn(t, carry):
        def one_block(b, inner):
            products = (
                mm_nt(right_all[t * each + b].reshape(factor * half, depth), left) * scaling
            ).astype(jnp.bfloat16)
            for e in range(factor):
                for g in range(lanes // 128):
                    outer[
                        pl.ds(pl.multiple_of(g * span + b * half, half), half),
                        e * 128 : (e + 1) * 128,
                    ] = products[e * half : (e + 1) * half, g * 128 : (g + 1) * 128]
            return inner

        lax.fori_loop(0, each, one_block, 0)
        pair = mm(outer[...], wpair_ref[...]).astype(jnp.bfloat16)

        def cut(i):
            g, k = i // pack, i % pack
            return pair[g * span : (g + 1) * span, k * channels : (k + 1) * channels]

        for i in range(own_rows):
            outgoing[t, i] = cut(own_rows + i)
        for i in range(own_rows):
            for b in range(each):
                start = pl.multiple_of((t * each + b) * residues + side * half, half)
                pair_ref[i, pl.ds(start, half), :] = cut(i)[b * half : (b + 1) * half]
        swap_copy(t).start()
        return carry

    lax.fori_loop(0, turns, one_turn, 0)

    def take(t, carry):
        swap_copy(t).wait_recv()
        for i in range(own_rows):
            for b in range(each):
                start = pl.multiple_of((t * each + b) * residues + (1 - side) * half, half)
                pair_ref[i, pl.ds(start, half), :] = incoming[t, i, b * half : (b + 1) * half, :]
        return carry

    lax.fori_loop(0, turns, take, 0)

    def drain(p, carry):
        cross(q, p, lax.rem(part_at(p) + half_parts, parts)).wait_send()
        direct(q, p, part_at(p)).wait_send()
        relay(across, p, part_at(p)).wait_send()
        return carry

    lax.fori_loop(0, parts, drain, 0)
    for way in range(2):

        def drain_ring(hop, carry):
            ring_copy(way, hop).wait_send()
            share_copy(way, hop).wait_send()
            return carry

        lax.fori_loop(0, ways[way], drain_ring, 0)

    def drain_swap(t, carry):
        swap_copy(t).wait_send()
        return carry

    lax.fori_loop(0, turns, drain_swap, 0)


def per_device(alignment, query_weight, w_keyval, w_gate, output_weight, w_factors, w_pair_out):
    seqs, residues, width = alignment.shape
    groups = lax.axis_size("seq")
    blocks = lax.axis_size("res")
    depth = seqs * groups
    factor = w_factors.shape[1] // 2
    channels = w_pair_out.shape[1]
    own_rows = residues // groups
    half = residues // 2
    parts = residues // COUNT
    hops = blocks // 2
    wft = jnp.transpose(w_factors)
    wqg = jnp.concatenate([query_weight, w_gate], axis=1)
    pack = 128 // factor
    w = jnp.transpose(w_pair_out.reshape(factor, factor, channels), (1, 0, 2))
    eye = jnp.eye(pack, dtype=w.dtype)
    spread = (w[:, None, :, None, :] * eye[None, :, None, :, None]).reshape(
        factor * pack * factor, pack * channels
    )
    each = math.gcd(blocks, 4)
    turns = blocks // each
    vmem = pl.BlockSpec(memory_space=pltpu.VMEM)
    dma = pltpu.SemaphoreType.DMA
    return pl.pallas_call(
        functools.partial(block_kernel, 1.0 / depth, blocks, groups),
        in_specs=[vmem] * 6,
        out_specs=[vmem] * 2,
        out_shape=[
            jax.ShapeDtypeStruct((seqs, residues, width), jnp.bfloat16),
            jax.ShapeDtypeStruct((own_rows, blocks * residues, channels), jnp.bfloat16),
        ],
        scratch_shapes=[
            pltpu.VMEM((groups, residues, seqs, width), jnp.bfloat16),
            pltpu.VMEM((width // 128, seqs * residues, 128), jnp.float32),
            pltpu.VMEM((depth // 128, factor * residues, 128), jnp.float32),
            pltpu.VMEM((residues, factor, depth), jnp.bfloat16),
            pltpu.VMEM((blocks, factor, half, depth), jnp.bfloat16),
            pltpu.VMEM((2 * own_rows * factor // 128 * each * half, factor * 128), jnp.bfloat16),
            pltpu.VMEM((turns, own_rows, each * half, channels), jnp.bfloat16),
            pltpu.VMEM((turns, own_rows, each * half, channels), jnp.bfloat16),
            dma((parts,)),
            dma((parts,)),
            dma((parts,)),
            dma((parts,)),
            dma((parts,)),
            dma((parts,)),
            dma((2, hops)),
            dma((2, hops)),
            dma((2, hops)),
            dma((2, hops)),
            dma((turns,)),
            dma((turns,)),
        ],
        compiler_params=pltpu.CompilerParams(
            vmem_limit_bytes=62 * 1024 * 1024, collective_id=0, has_side_effects=True
        ),
        name="block",
    )(alignment, wqg, w_keyval, output_weight, wft, spread)


def solution(mesh):
    in_specs = (P("seq", "res", None), P(), P(), P(), P(), P(), P())
    out_specs = (P("seq", "res", None), P(("res", "seq"), None, None))
    return jax.shard_map(
        per_device, mesh=mesh, in_specs=in_specs, out_specs=out_specs, check_vma=False
    )
```

```python
import functools
import math

import jax
import jax.numpy as jnp
from jax import lax
from jax.experimental import pallas as pl
from jax.experimental.pallas import tpu as pltpu
from jax.sharding import PartitionSpec as P

HEADS = 8
HC = 32
LOG2E = 1.4426950408889634
epsilon = 1e-05
NT = (((1,), (1,)), ((), ()))


def mm(a, b):
    return jnp.dot(a, b, preferred_element_type=jnp.float32)


def mm_nt(a, b):
    return lax.dot_general(a, b, NT, preferred_element_type=jnp.float32)


MESH = pl.DeviceIdType.MESH
COUNT = 4


def attend_residues(own, everything, wq, wg, wkv, wout):
    groups, count, seqs, width = everything.shape
    hidden = HEADS * HC
    kv = mm(everything.reshape(groups * count * seqs, width), wkv).astype(jnp.bfloat16)
    kv = kv.reshape(groups, count, seqs, 2 * hidden)
    rows = own.reshape(count * seqs, width)
    queries = mm(rows, wq).astype(jnp.bfloat16)
    gating = jax.nn.sigmoid(mm(rows, wg))
    head_of = lax.broadcasted_iota(jnp.int32, (seqs, hidden), 1) // HC
    gated = []
    for n in range(count):
        q = queries[n * seqs : (n + 1) * seqs].astype(jnp.float32)
        stacked = jnp.concatenate(
            [jnp.where(head_of == h, q, 0.0).astype(jnp.bfloat16) for h in range(HEADS)], axis=0
        )
        keys = kv[:, n, :, :hidden].reshape(groups * seqs, hidden)
        values = kv[:, n, :, hidden:].reshape(groups * seqs, hidden)
        exponent = jnp.exp2(mm_nt(stacked, keys) * (LOG2E / math.sqrt(HC)))
        inverse = 1.0 / jnp.sum(exponent, axis=-1, keepdims=True)
        weighted = mm(exponent.astype(jnp.bfloat16), values)
        attended = jnp.zeros((seqs, hidden), jnp.float32)
        for h in range(HEADS):
            rows = slice(h * seqs, (h + 1) * seqs)
            attended = jnp.where(head_of == h, weighted[rows] * inverse[rows], attended)
        gated.append((gating[n * seqs : (n + 1) * seqs] * attended).astype(jnp.bfloat16))
    return mm(jnp.concatenate(gated, axis=0), wout)


def block_kernel(
    scaling,
    blocks,
    groups,
    x_ref,
    wq_ref,
    wkv_ref,
    wg_ref,
    wout_ref,
    wf_ref,
    wp_ref,
    o_ref,
    pair_ref,
    gathered,
    strided,
    pair_rows,
    spread,
    wft,
    left_all,
    right_all,
    products,
    outer,
    outgoing,
    incoming,
    cross_send,
    cross_recv,
    twin_send,
    twin_recv,
    relay_send,
    relay_recv,
    ring_send,
    ring_recv,
    share_send,
    share_recv,
    swap_send,
    swap_recv,
):
    seqs, residues, width = x_ref.shape
    depth = seqs * groups
    factor = wf_ref.shape[1] // 2
    pack = 128 // factor
    own_rows = residues // groups
    channels = pair_ref.shape[2]
    half = residues // 2
    parts = residues // COUNT
    half_parts = parts // 2
    hops = blocks // 2
    r = lax.axis_index("res")
    q = lax.axis_index("seq")
    core = lax.rem(q, 2)
    side = q // 2
    twin = q + 1 - 2 * core
    across = lax.rem(q + 2, groups)
    twin_across = lax.rem(twin + 2, groups)

    def ring_of(block):
        z, y = block // 2, lax.rem(block, 2)
        return jnp.where(y == 0, z, blocks - 1 - z)

    def block_of(place):
        return jnp.where(place < blocks // 2, 2 * place, 2 * (blocks - 1 - place) + 1)

    place = ring_of(r)
    ahead = block_of(lax.rem(place + 1, blocks))
    behind = block_of(lax.rem(place + blocks - 1, blocks))

    barrier = pltpu.get_barrier_semaphore()
    for target in ((r, twin), (r, across), (ahead, q), (behind, q)):
        pl.semaphore_signal(barrier, inc=1, device_id=target, device_id_type=MESH)
    pl.semaphore_wait(barrier, 4)

    def part_at(p):
        return lax.rem(p + side * half_parts, parts)

    def rows_of(owner, part):
        return gathered.at[owner, pl.ds(part * COUNT, COUNT)]

    def send(ref, dst, send_sem, recv_sem, target):
        return pltpu.make_async_remote_copy(
            src_ref=ref,
            dst_ref=dst,
            send_sem=send_sem,
            recv_sem=recv_sem,
            device_id=target,
            device_id_type=MESH,
        )

    def cross(owner, p, part):
        block = rows_of(owner, part)
        return send(block, block, cross_send.at[p], cross_recv.at[p], (r, across))

    def direct(owner, p, part):
        block = rows_of(owner, part)
        return send(block, block, twin_send.at[p], twin_recv.at[p], (r, twin))

    def relay(owner, p, part):
        block = rows_of(owner, part)
        return send(block, block, relay_send.at[p], relay_recv.at[p], (r, twin))

    step = 8
    for turn in range(2):
        which = (1 - side) if turn == 0 else side
        base = pl.multiple_of(which * half, half)

        def norm(i, carry):
            values = (
                x_ref[pl.ds(i * step, step), pl.ds(base, half), :]
                .reshape(step * half, width)
                .astype(jnp.float32)
            )
            centered = values - jnp.mean(values, axis=-1, keepdims=True)
            spread = jnp.mean(centered * centered, axis=-1, keepdims=True)
            normed = centered * lax.rsqrt(spread + epsilon)
            for part in range(width // 128):
                strided[part, pl.ds(i * (step * half), step * half), :] = normed[
                    :, part * 128 : (part + 1) * 128
                ]
            return carry

        lax.fori_loop(0, seqs // step, norm, 0)

        def move(k, carry):
            for n in range(COUNT):
                for part in range(width // 128):
                    gathered[q, base + k * COUNT + n, :, part * 128 : (part + 1) * 128] = strided[
                        part, pl.ds(k * COUNT + n, seqs, half), :
                    ].astype(jnp.bfloat16)
            return carry

        def start_across(k, carry):
            cross(q, turn * half_parts + k, which * half_parts + k).start()
            return carry

        def move_and_start(k, carry):
            move(k, carry)
            return start_across(k, carry)

        lax.fori_loop(0, half_parts, move_and_start, 0)

    def start_twin(p, carry):
        direct(q, p, part_at(p)).start()
        return carry

    lax.fori_loop(0, parts, start_twin, 0)

    both_factors = 2 * factor
    unit = jnp.where(
        lax.broadcasted_iota(jnp.int32, (both_factors, both_factors), 0)
        == lax.broadcasted_iota(jnp.int32, (both_factors, both_factors), 1),
        1.0,
        0.0,
    ).astype(jnp.bfloat16)
    wft[...] = mm_nt(unit, wf_ref[...]).astype(jnp.bfloat16)
    pair_rows[...] = wp_ref[...].astype(jnp.float32)
    spread[...] = jnp.zeros_like(spread)
    for e in range(factor):
        rows = pair_rows[pl.ds(e, factor, factor), :].astype(jnp.bfloat16)
        for k in range(pack):
            start = (e * pack + k) * factor
            spread[start : start + factor, k * channels : (k + 1) * channels] = rows

    share = COUNT // 2

    def mine(sub):
        return pl.ds(sub * COUNT + core * share, share)

    def twins(sub):
        return pl.ds(sub * COUNT + (1 - core) * share, share)

    def ring_copy(way, sub, hop):
        shift = blocks - hop if way == 0 else hop
        block = block_of(lax.rem(place + shift, blocks))
        ref = right_all.at[block, mine(sub)]
        return send(
            ref,
            ref,
            ring_send.at[way, sub, hop],
            ring_recv.at[way, sub, hop],
            ((ahead if way == 0 else behind), q),
        )

    def landed(way, hop):
        shift = blocks - hop - 1 if way == 0 else hop + 1
        return block_of(lax.rem(place + shift, blocks))

    def arrive(way, sub, hop):
        ref = right_all.at[landed(way, hop), mine(sub)]
        send(
            ref,
            ref,
            ring_send.at[way, sub, hop],
            ring_recv.at[way, sub, hop],
            ((ahead if way == 0 else behind), q),
        ).wait_recv()

    def share_copy(way, sub, hop, outward=True):
        ref = right_all.at[landed(way, hop), mine(sub) if outward else twins(sub)]
        return send(
            ref, ref, share_send.at[way, sub, hop], share_recv.at[way, sub, hop], (r, twin)
        )

    ways = (hops, blocks - 1 - hops)

    def advance(sub, hop):
        for way in range(2):

            @pl.when((hop > 0) & (hop <= ways[way]))
            def _():
                arrive(way, sub, hop - 1)

            @pl.when((hop >= 0) & (hop < ways[way]))
            def _():
                ring_copy(way, sub, hop).start()

            @pl.when((hop > 0) & (hop <= ways[way]))
            def _():
                share_copy(way, sub, hop - 1).start()

    def advance_all(p):
        for sub in range(half_parts):
            advance(sub, p - sub)

    def one_part(p, carry):
        part = part_at(p)
        cross(across, p, part).wait_recv()
        relay(across, p, part).start()
        direct(twin, p, part).wait_recv()
        relay(twin_across, p, part).wait_recv()
        everything = gathered[:, pl.ds(part * COUNT, COUNT)]
        for n in range(COUNT):
            both = mm_nt(wft[...], everything[:, n].reshape(depth, width)).astype(jnp.bfloat16)
            left_all[part * COUNT + n] = both[:factor]

            @pl.when(p < half_parts)
            def _():
                right_all[r, p * COUNT + n] = both[factor:]

        update = attend_residues(
            gathered[q, pl.ds(part * COUNT, COUNT)],
            everything,
            wq_ref[...],
            wg_ref[...],
            wkv_ref[...],
            wout_ref[...],
        )
        for n in range(COUNT):
            for piece in range(width // 128):
                strided[piece, pl.ds(part * COUNT + n, seqs, residues), :] = update[
                    n * seqs : (n + 1) * seqs, piece * 128 : (piece + 1) * 128
                ]

        advance_all(p)
        return carry

    lax.fori_loop(0, parts, one_part, 0)

    def late(p, carry):
        advance_all(p)
        return carry

    lax.fori_loop(parts, half_parts + hops, late, 0)

    for way in range(2):
        for sub in range(half_parts):

            def shared(hop, carry):
                share_copy(way, sub, hop, False).wait_recv()
                return carry

            lax.fori_loop(0, ways[way], shared, 0)

    lanes = own_rows * factor
    span = blocks * half

    def pair_of(owner):
        left = left_all[pl.ds(owner * own_rows, own_rows)].reshape(lanes, depth)

        def one_block(b, inner):
            value = mm_nt(right_all[b].reshape(half * factor, depth), left) * scaling
            for g in range(lanes // 128):
                products[g] = value[:, g * 128 : (g + 1) * 128]
            for e in range(factor):
                for g in range(lanes // 128):
                    outer[
                        pl.ds(pl.multiple_of(g * span + b * half, half), half),
                        e * 128 : (e + 1) * 128,
                    ] = products[g, pl.ds(e, half, factor), :].astype(jnp.bfloat16)
            return inner

        lax.fori_loop(0, blocks, one_block, 0)
        return mm(outer[...], spread[...]).astype(jnp.bfloat16)

    def cut(pair, i):
        g, k = i // pack, i % pack
        return pair[g * span : (g + 1) * span, k * channels : (k + 1) * channels]

    def swap_copy():
        return send(outgoing, incoming, swap_send, swap_recv, (r, across))

    pair = pair_of(across)
    for i in range(own_rows):
        outgoing[i] = cut(pair, i)
    swap_copy().start()

    def place_rows(i, which, value):
        for b in range(blocks):
            start = pl.multiple_of(b * residues + which * half, half)
            pair_ref[i, pl.ds(start, half), :] = value[b * half : (b + 1) * half]

    pair = pair_of(q)
    for i in range(own_rows):
        place_rows(i, side, cut(pair, i))

    def finish(i, carry):
        for piece in range(width // 128):
            o_ref[pl.ds(i * step, step), :, piece * 128 : (piece + 1) * 128] = (
                strided[piece, pl.ds(i * (step * residues), step * residues), :]
                .astype(jnp.bfloat16)
                .reshape(step, residues, 128)
            )
        return carry

    lax.fori_loop(0, seqs // step, finish, 0)
    swap_copy().wait_recv()
    for i in range(own_rows):
        place_rows(i, 1 - side, incoming[i])

    def drain(p, carry):
        cross(q, p, lax.rem(part_at(p) + half_parts, parts)).wait_send()
        direct(q, p, part_at(p)).wait_send()
        relay(across, p, part_at(p)).wait_send()
        return carry

    lax.fori_loop(0, parts, drain, 0)
    for way in range(2):
        for sub in range(half_parts):

            def drain_ring(hop, carry):
                ring_copy(way, sub, hop).wait_send()
                share_copy(way, sub, hop).wait_send()
                return carry

            lax.fori_loop(0, ways[way], drain_ring, 0)
    swap_copy().wait_send()


def per_device(alignment, query_weight, w_keyval, w_gate, output_weight, w_factors, w_pair_out):
    seqs, residues, width = alignment.shape
    groups = lax.axis_size("seq")
    blocks = lax.axis_size("res")
    depth = seqs * groups
    factor = w_factors.shape[1] // 2
    channels = w_pair_out.shape[1]
    own_rows = residues // groups
    half = residues // 2
    parts = residues // COUNT
    hops = blocks // 2
    pack = 128 // factor
    subs = parts // 2
    span = blocks * half
    vmem = pl.BlockSpec(memory_space=pltpu.VMEM)
    dma = pltpu.SemaphoreType.DMA
    return pl.pallas_call(
        functools.partial(block_kernel, 1.0 / depth, blocks, groups),
        in_specs=[vmem] * 7,
        out_specs=[vmem] * 2,
        out_shape=[
            jax.ShapeDtypeStruct((seqs, residues, width), jnp.bfloat16),
            jax.ShapeDtypeStruct((own_rows, blocks * residues, channels), jnp.bfloat16),
        ],
        scratch_shapes=[
            pltpu.VMEM((groups, residues, seqs, width), jnp.bfloat16),
            pltpu.VMEM((width // 128, seqs * residues, 128), jnp.float32),
            pltpu.VMEM((factor * factor, channels), jnp.float32),
            pltpu.VMEM((factor * 128, pack * channels), jnp.bfloat16),
            pltpu.VMEM((2 * factor, width), jnp.bfloat16),
            pltpu.VMEM((residues, factor, depth), jnp.bfloat16),
            pltpu.VMEM((blocks, half, factor, depth), jnp.bfloat16),
            pltpu.VMEM((own_rows // pack, half * factor, 128), jnp.float32),
            pltpu.VMEM((own_rows // pack * span, factor * 128), jnp.bfloat16),
            pltpu.VMEM((own_rows, span, channels), jnp.bfloat16),
            pltpu.VMEM((own_rows, span, channels), jnp.bfloat16),
            dma((parts,)),
            dma((parts,)),
            dma((parts,)),
            dma((parts,)),
            dma((parts,)),
            dma((parts,)),
            dma((2, subs, hops)),
            dma((2, subs, hops)),
            dma((2, subs, hops)),
            dma((2, subs, hops)),
            dma,
            dma,
        ],
        compiler_params=pltpu.CompilerParams(
            vmem_limit_bytes=62 * 1024 * 1024, collective_id=0, has_side_effects=True
        ),
        name="block",
    )(alignment, query_weight, w_keyval, w_gate, output_weight, w_factors, w_pair_out)


def solution(mesh):
    in_specs = (P("seq", "res", None), P(), P(), P(), P(), P(), P())
    out_specs = (P("seq", "res", None), P(("res", "seq"), None, None))
    return jax.shard_map(
        per_device, mesh=mesh, in_specs=in_specs, out_specs=out_specs, check_vma=False
    )
```
